32 devices in a mesh: dp: 8 (over z, x), col: 4 (over y, core).
Axes of the slice: x: 2, y: 2, z: 4, core: 2. Of those that a mesh axis runs over, the one named last changes fastest.
Arguments:
- activations: bfloat16 [2, 7168, 8192], P(None, 'dp', 'col'), may hold values from -40 to 40
- cotangent: bfloat16 [2, 7168, 2048], P(None, 'dp'), may hold values from -40 to 40
- master_weights: float32 [2, 2048, 8192], P(None, 'dp', 'col'), may hold values from -6 to 6
- moment_codes: bfloat16 [2, 2048, 8192], P(None, 'dp', 'col'), may hold values from -1 to 1
- square_codes: bfloat16 [2, 2048, 8192], P(None, 'dp', 'col'), may hold values from 0.049804688 to 1
- moment_scales: float32 [2, 2048, 4], P(None, 'dp'), may hold values from 0.05 to 0.5
- square_scales: float32 [2, 2048, 4], P(None, 'dp'), may hold values from 0.005 to 0.05
Outputs:
- new_weights: float32 [2, 2048, 8192], P(None, 'dp', 'col')
- new_moment_codes: bfloat16 [2, 2048, 8192], P(None, 'dp', 'col')
- new_square_codes: bfloat16 [2, 2048, 8192], P(None, 'dp', 'col')
- new_moment_scales: float32 [2, 2048, 4], P(None, 'dp')
- new_square_scales: float32 [2, 2048, 4], P(None, 'dp')
The draws below stay inside these ranges and needn't reach their ends.
All inputs are finite; a program needn't handle non-finite values. Where the reference program divides by a largest or mean magnitude, that divisor is 1e-20 or more.
Results may differ from the reference program's by a relative error of at most 0.001.
Values sent between devices are 32-bit elements; how exact they have to be, the bound alone decides.
A program may use at most 128 MiB of HBM per device.

```python
import math
import jax
import jax.numpy as jnp
from jax import lax

D = 8192
KV = 2048
BLOCK = 2048
LAYERS = 2
STEP = 10
TOK_DEV = 896
TOKENS = 7168
NB = 4
N_DP = 8


def scaled_values(key, width):
    keys = jax.random.split(key, 2)
    position = jnp.arange(width, dtype=jnp.float32) / width
    col_scale = jnp.exp(jnp.log(3.0) * position + jnp.log(3.4) * jax.random.uniform(keys[1], (width,)))
    values = jax.random.normal(keys[0], (LAYERS, TOKENS, width)) * col_scale
    return jnp.clip(values, -40.0, 40.0).astype(jnp.bfloat16)


def draw_activations(key, part):
    return scaled_values(jax.random.fold_in(key, 11), D)


def draw_cotangent(key, part):
    return scaled_values(jax.random.fold_in(key, 23), KV)


def shard_levels(stream_key, shape, cuts, smallest, high):
    def one(axis_at, parts):
        heights = jax.random.uniform(jax.random.fold_in(jax.random.fold_in(stream_key, 6), axis_at), (parts,), jnp.float32, smallest / len(cuts), high / len(cuts))
        return jnp.repeat(jnp.exp(heights), shape[axis_at] // parts).reshape((-1,) + (1,) * (len(shape) - axis_at - 1))

    gain = one(*cuts[0])
    for cut in cuts[1:]:
        gain = gain * one(*cut)
    return gain


def normal_values(stream_key, shape, scale, limit, shards=(), kind=jnp.bfloat16):
    array = scale * jax.random.normal(stream_key, shape, jnp.float32)
    if shards:
        array = array * shard_levels(stream_key, shape, shards, -0.22, 0.18)
    return jnp.clip(array, -limit, limit).astype(kind)


def setup_inputs(seed: int = 0) -> dict:
    arg_keys = jax.random.split(jax.random.key(seed), 8)
    return {
        "activations": draw_activations(jax.random.fold_in(arg_keys[7], 71), 0),
        "cotangent": draw_cotangent(jax.random.fold_in(arg_keys[7], 71), 0),
        "master_weights": normal_values(arg_keys[2], (LAYERS, KV, D), 1.0, 6.0, ((1, 8), (2, 4)), jnp.float32),
        "moment_codes": jnp.clip(jax.random.uniform(arg_keys[3], (LAYERS, KV, D), jnp.float32, -1.0, 1.0) * shard_levels(arg_keys[3], (LAYERS, KV, D), ((1, 8), (2, 4)), -0.4, 0.0), -1.0, 1.0).astype(jnp.bfloat16),
        "square_codes": jnp.clip(0.049804688 + 0.9501953 * jax.random.uniform(arg_keys[4], (LAYERS, KV, D), jnp.float32) ** shard_levels(arg_keys[4], (LAYERS, KV, D), ((1, 8), (2, 4)), -0.2, 0.2), 0.049804688, 1.0).astype(jnp.bfloat16),
        "moment_scales": jnp.clip(jnp.exp(math.log(0.5) - 2.3025851 * jax.random.uniform(arg_keys[5], (LAYERS, KV, NB), jnp.float32) ** shard_levels(arg_keys[5], (LAYERS, KV, NB), ((1, 8),), -0.2, 0.2)), 0.05, 0.5),
        "square_scales": jnp.clip(jnp.exp(math.log(0.05) - 2.3025851 * jax.random.uniform(arg_keys[6], (LAYERS, KV, NB), jnp.float32) ** shard_levels(arg_keys[6], (LAYERS, KV, NB), ((1, 8),), -0.2, 0.2)), 0.005, 0.05),
    }


beta_one = 0.9
beta_two = 0.999
learn_rate = 0.001
decay_rate = 0.1
adam_eps = 1e-08
scale_eps = 1e-06
norm_eps = 1e-06

def layer_gradient(layer_acts, layer_cot):
    grouped_acts = layer_acts.reshape(N_DP, TOK_DEV, D)
    grouped_cot = layer_cot.reshape(N_DP, TOK_DEV, KV)

    def accumulate(total, pair):
        group_acts, group_cot = pair
        partial_sum = lax.dot_general(group_cot, group_acts, (((0,), (0,)), ((), ())), preferred_element_type=jnp.float32)
        return (total + partial_sum, None)
    total, unused = lax.scan(accumulate, jnp.zeros((KV, D), jnp.float32), (grouped_acts, grouped_cot))
    return total

def reference(activations, cotangent, master_weights, moment_codes, square_codes, moment_scales, square_scales):
    gradients = [layer_gradient(activations[index], cotangent[index]) for index in range(LAYERS)]
    total_sq = jnp.float32(0.0)
    for gradient in gradients:
        total_sq = total_sq + jnp.sum(gradient * gradient)
    rms = jnp.sqrt(total_sq / float(LAYERS * KV * D) + norm_eps)
    clip_factor = jnp.minimum(1.0, 1.0 / rms)
    correct_one = 1.0 - beta_one ** STEP
    correct_two = 1.0 - beta_two ** STEP
    outs_weights, outs_mcode, outs_scode, outs_mscale, outs_sscale = ([], [], [], [], [])
    for index in range(LAYERS):
        old_moment = moment_codes[index].astype(jnp.float32).reshape(KV, NB, BLOCK) * moment_scales[index][:, :, None]
        old_square = square_codes[index].astype(jnp.float32).reshape(KV, NB, BLOCK) * square_scales[index][:, :, None]
        grad_now = (clip_factor * gradients[index]).reshape(KV, NB, BLOCK)
        moment = beta_one * old_moment + (1.0 - beta_one) * grad_now
        square = beta_two * old_square + (1.0 - beta_two) * grad_now * grad_now
        moment_max = lax.optimization_barrier(jnp.max(jnp.abs(moment), axis=2))
        square_max = lax.optimization_barrier(jnp.max(square, axis=2))
        outs_mcode.append((moment / (moment_max[:, :, None] + scale_eps)).astype(jnp.bfloat16).reshape(KV, D))
        outs_scode.append((square / (square_max[:, :, None] + scale_eps)).astype(jnp.bfloat16).reshape(KV, D))
        outs_mscale.append(moment_max)
        outs_sscale.append(square_max)
        ratio = (moment / correct_one / (jnp.sqrt(square / correct_two) + adam_eps)).reshape(KV, D)
        weights = master_weights[index]
        outs_weights.append(weights - learn_rate * (decay_rate * weights + ratio))
    return (jnp.stack(outs_weights), jnp.stack(outs_mcode), jnp.stack(outs_scode), jnp.stack(outs_mscale), jnp.stack(outs_sscale))
```

```python
import functools

import jax
import jax.numpy as jnp
from jax import lax
from jax.experimental import pallas as pl
from jax.experimental.pallas import tpu as pltpu
from jax.sharding import PartitionSpec as P

D = 8192
KV = 2048
BLOCK = 2048
LAYERS = 2
STEP = 10


beta_one = 0.9
beta_two = 0.999
learn_rate = 0.001
decay_rate = 0.1
adam_eps = 1e-08
scale_eps = 1e-06
norm_eps = 1e-06

LANES = 128
AHEAD = 3
XSLOTS = 4


def reduce_kernel(
    count, col_count, cot_ref, act_ref, out_ref, sq_ref,
    xs, xr, part, arr, bs, br, own_sq, sum_sq, col_sq, dp_sq,
    xs_sem, xr_sem, rs_sem, rr_sem, ls_sem, ll_sem, bs_sem, br_sem,
    cs_sem, cr_sem, ds_sem, dr_sem, x_free, from_right, from_left,
):
    layers, pairs, line, rows, tokens = cot_ref.shape
    cols = act_ref.shape[2]
    slots = part.shape[0]
    wide_per = cols // (2 * LANES) - 1
    per_layer = wide_per + 2
    period = (per_layer + 1) // 2
    items = layers * per_layer
    wides = layers * wide_per
    me = lax.axis_index("dp")
    z = me // 2
    x = me % 2
    peer = 2 * z + 1 - x
    right = jnp.minimum(z + 1, line - 1) * 2 + x
    left = jnp.maximum(z - 1, 0) * 2 + x
    has_right = z < line - 1
    has_left = z > 0
    mirror = line - 1 - z

    def signal(sem, where):
        pl.semaphore_signal(
            sem, inc=1, device_id={"dp": where}, device_id_type=pl.DeviceIdType.MESH
        )

    barrier = pltpu.get_barrier_semaphore()
    mine = lax.axis_index("col")
    for offset in range(1, count):
        signal(barrier, lax.rem(me + offset, count))
    for offset in range(1, col_count):
        pl.semaphore_signal(
            barrier, inc=1, device_id={"col": lax.rem(mine + offset, col_count)},
            device_id_type=pl.DeviceIdType.MESH,
        )
    pl.semaphore_wait(barrier, count + col_count - 2)

    def remote(src, dst, send, recv, where):
        return pltpu.make_async_remote_copy(
            src_ref=src, dst_ref=dst, send_sem=send, recv_sem=recv,
            device_id={"dp": where}, device_id_type=pl.DeviceIdType.MESH,
        )

    def describe(item):
        layer = item // per_layer
        place = item % per_layer
        narrow = place % period == 0
        wide_at = place - (place + period - 1) // period
        narrow_at = place // period
        return layer, narrow, wide_at, narrow_at

    def x_copy(number):
        slot = number % XSLOTS
        return remote(xs.at[slot], xr.at[slot], xs_sem.at[slot], xr_sem.at[slot], peer)

    def r_copy(slot, target):
        return remote(
            part.at[slot, target], arr.at[slot, target + 1],
            rs_sem.at[slot, target], rr_sem.at[slot, target], right,
        )

    def l_copy(slot, target):
        return remote(
            part.at[slot, target], arr.at[slot, target],
            ls_sem.at[slot, target], ll_sem.at[slot, target], left,
        )

    def b_copy(number):
        return remote(
            bs.at[number], br.at[number], bs_sem.at[number], br_sem.at[number], peer
        )

    def product(layer, pair, target, start, width):
        return jnp.dot(
            cot_ref[layer, pair, target],
            act_ref[layer, :, pl.ds(pl.multiple_of(start, LANES), width)],
            preferred_element_type=jnp.float32,
        )

    def send_wide(item):
        layer, narrow, wide_at, _ = describe(item)

        @pl.when(jnp.logical_not(narrow))
        def _():
            number = layer * wide_per + wide_at
            slot = number % XSLOTS

            @pl.loop(0, line)
            def _(target):
                value = product(layer, 1 - x, target, wide_at * 2 * LANES, 2 * LANES)
                xs[slot, target, 0] = value[:, :LANES]
                xs[slot, target, 1] = value[:, LANES:]

            @pl.when(number >= XSLOTS)
            def _():
                pl.semaphore_wait(x_free, 1)

            x_copy(number).start()

    def form(item):
        layer, narrow, wide_at, narrow_at = describe(item)
        here = item % slots

        @pl.when(item >= slots)
        def _():
            @pl.when(has_right)
            def _():
                pl.semaphore_wait(from_right, 1)

            @pl.when(has_left)
            def _():
                pl.semaphore_wait(from_left, 1)

        @pl.when(narrow)
        def _():
            start = wide_per * 2 * LANES + narrow_at * LANES

            @pl.loop(0, line)
            def _(target):
                part[here, target, 0] = product(layer, 0, target, start, LANES)
                part[here, target, 1] = product(layer, 1, target, start, LANES)

        @pl.when(jnp.logical_not(narrow))
        def _():
            number = layer * wide_per + wide_at
            slot = number % XSLOTS
            x_copy(number).wait()

            @pl.loop(0, line)
            def _(target):
                value = product(layer, x, target, wide_at * 2 * LANES, 2 * LANES)
                part[here, target, 0] = value[:, :LANES] + xr[slot, target, 0]
                part[here, target, 1] = value[:, LANES:] + xr[slot, target, 1]

            @pl.when(number + XSLOTS < wides)
            def _():
                signal(x_free, peer)

    def hop(item, stage):
        here = item % slots

        @pl.when(z <= stage)
        def _():
            target = line - 1 - stage + z
            if stage > 0:
                @pl.when(has_left)
                def _():
                    r_copy(here, target).wait_recv()
                    part[here, target] += arr[here, target + 1]

            r_copy(here, target).start()

        @pl.when(mirror <= stage)
        def _():
            target = stage - mirror
            if stage > 0:
                @pl.when(has_right)
                def _():
                    l_copy(here, target).wait_recv()
                    part[here, target] += arr[here, target]

            l_copy(here, target).start()

    def finish(item):
        layer, narrow, wide_at, narrow_at = describe(item)
        here = item % slots

        @pl.when(has_left)
        def _():
            r_copy(here, z).wait_recv()
            part[here, z] += arr[here, z + 1]

        @pl.when(has_right)
        def _():
            l_copy(here, z).wait_recv()
            part[here, z] += arr[here, z]

        for target in range(line):
            @pl.when(target > z)
            def _(target=target):
                r_copy(here, target).wait_send()

            @pl.when(target < z)
            def _(target=target):
                l_copy(here, target).wait_send()

        @pl.when(narrow)
        def _():
            number = layer * 2 + narrow_at
            start = wide_per * 2 * LANES + narrow_at * LANES
            bs[number] = part[here, z, 1 - x]
            b_copy(number).start()
            out_ref[layer, :, pl.ds(pl.multiple_of(start, LANES), LANES)] = part[here, z, x]

        @pl.when(jnp.logical_not(narrow))
        def _():
            for half in range(2):
                start = wide_at * 2 * LANES + half * LANES
                out_ref[layer, :, pl.ds(pl.multiple_of(start, LANES), LANES)] = part[here, z, half]

        @pl.when(item + slots < items)
        def _():
            @pl.when(has_left)
            def _():
                signal(from_right, left)

            @pl.when(has_right)
            def _():
                signal(from_left, right)

    for item in range(1, AHEAD):
        send_wide(jnp.int32(item))

    @pl.loop(0, items + line - 1)
    def _(step):
        def guard(item, action):
            pl.when(jnp.logical_and(item >= 0, item < items))(lambda: action(item))

        guard(step + AHEAD, send_wide)
        guard(step - (line - 1), finish)
        for stage in reversed(range(1, line - 1)):
            guard(step - stage, functools.partial(hop, stage=stage))

        def begin(item):
            form(item)
            hop(item, 0)

        guard(step, begin)

    for number in range(2 * layers):
        b_copy(number).wait()
        start = wide_per * 2 * LANES + (number % 2) * LANES
        out_ref[number // 2, :, start : start + LANES] += br[number]

    def square_rows(index, total):
        layer = index // (rows // 8)
        at = pl.multiple_of(index % (rows // 8) * 8, 8)
        for piece in range(cols // LANES):
            value = out_ref[layer, pl.ds(at, 8), piece * LANES : (piece + 1) * LANES]
            total = total + value * value
        return total

    def spread(src, landing, send, recv, axis, index, size):
        copies = []
        for offset in range(1, size):
            copies.append(
                pltpu.make_async_remote_copy(
                    src_ref=src, dst_ref=landing.at[offset - 1],
                    send_sem=send.at[offset - 1], recv_sem=recv.at[offset - 1],
                    device_id={axis: lax.rem(index + offset, size)},
                    device_id_type=pl.DeviceIdType.MESH,
                )
            )
        for copy in copies:
            copy.start()
        for copy in copies:
            copy.wait()
        total = src[...]
        for offset in range(1, size):
            total = total + landing[offset - 1]
        return total

    own_sq[...] = lax.fori_loop(
        0, layers * rows // 8, square_rows, jnp.zeros((8, LANES), jnp.float32)
    )
    sum_sq[...] = spread(own_sq, col_sq, cs_sem, cr_sem, "col", mine, col_count)
    sq_ref[...] = spread(sum_sq, dp_sq, ds_sem, dr_sem, "dp", me, count)


def reduced_gradient(activations, cotangent, mesh_shape):
    count = mesh_shape["dp"]
    col_count = mesh_shape["col"]
    layers, tokens, cols = activations.shape
    line = count // 2
    rows = cotangent.shape[2] // count
    slots = line + 2
    cot = cotangent.reshape(layers, tokens, line, 2, rows).transpose(0, 3, 2, 4, 1)
    block = (line, 2, rows, LANES)
    dma = pltpu.SemaphoreType.DMA
    vmem = pl.BlockSpec(memory_space=pltpu.VMEM)
    return pl.pallas_call(
        functools.partial(reduce_kernel, count, col_count),
        out_shape=(
            jax.ShapeDtypeStruct((layers, rows, cols), jnp.float32),
            jax.ShapeDtypeStruct((8, LANES), jnp.float32),
        ),
        in_specs=[vmem, vmem],
        out_specs=(vmem, vmem),
        scratch_shapes=[
            pltpu.VMEM((XSLOTS,) + block, jnp.float32),
            pltpu.VMEM((XSLOTS,) + block, jnp.float32),
            pltpu.VMEM((slots,) + block, jnp.float32),
            pltpu.VMEM((slots, line + 1) + block[1:], jnp.float32),
            pltpu.VMEM((2 * layers, rows, LANES), jnp.float32),
            pltpu.VMEM((2 * layers, rows, LANES), jnp.float32),
            pltpu.VMEM((8, LANES), jnp.float32),
            pltpu.VMEM((8, LANES), jnp.float32),
            pltpu.VMEM((col_count - 1, 8, LANES), jnp.float32),
            pltpu.VMEM((count - 1, 8, LANES), jnp.float32),
            dma((XSLOTS,)), dma((XSLOTS,)),
            dma((slots, line)), dma((slots, line)), dma((slots, line)), dma((slots, line)),
            dma((2 * layers,)), dma((2 * layers,)),
            dma((col_count - 1,)), dma((col_count - 1,)), dma((count - 1,)), dma((count - 1,)),
            pltpu.SemaphoreType.REGULAR, pltpu.SemaphoreType.REGULAR, pltpu.SemaphoreType.REGULAR,
        ],
        compiler_params=pltpu.CompilerParams(
            collective_id=0, has_side_effects=True, vmem_limit_bytes=62 * 2**20
        ),
    )(cot, activations)


def local(
    mesh_shape, activations, cotangent, master_weights, moment_codes, square_codes, moment_scales, square_scales
):
    layer_count = activations.shape[0]
    shard_rows = master_weights.shape[1]
    shard_cols = master_weights.shape[2]
    block_count = moment_scales.shape[2]
    gradient, squares = reduced_gradient(activations, cotangent, mesh_shape)
    total_sq = jnp.sum(squares)
    rms = jnp.sqrt(total_sq / float(LAYERS * KV * D) + norm_eps)
    clip_factor = jnp.minimum(1.0, 1.0 / rms)
    correct_one = 1.0 - beta_one**STEP
    correct_two = 1.0 - beta_two**STEP
    own_block = lax.axis_index("col") * shard_cols // BLOCK
    selector = (jnp.arange(block_count, dtype=jnp.int32) == own_block).astype(jnp.float32)
    outs_weights, outs_mcode, outs_scode, outs_mscale, outs_sscale = ([], [], [], [], [])
    for layer_index in range(layer_count):
        moment_scale = jnp.sum(moment_scales[layer_index] * selector, axis=1)
        square_scale = jnp.sum(square_scales[layer_index] * selector, axis=1)
        old_moment = moment_codes[layer_index].astype(jnp.float32) * moment_scale[:, None]
        old_square = square_codes[layer_index].astype(jnp.float32) * square_scale[:, None]
        grad_now = clip_factor * gradient[layer_index]
        new_moment = beta_one * old_moment + (1.0 - beta_one) * grad_now
        new_square = beta_two * old_square + (1.0 - beta_two) * grad_now * grad_now
        moment_part = jnp.max(jnp.abs(new_moment), axis=1)[:, None] * selector
        square_part = jnp.max(new_square, axis=1)[:, None] * selector
        moment, square, moment_part, square_part = (
            new_moment,
            new_square,
            moment_part,
            square_part,
        )
        moment_max, square_max = lax.pmax((moment_part, square_part), "col")
        moment_div = jnp.sum(moment_max * selector, axis=1)[:, None]
        square_div = jnp.sum(square_max * selector, axis=1)[:, None]
        moment_out = (moment / (moment_div + scale_eps)).astype(jnp.bfloat16)
        square_out = (square / (square_div + scale_eps)).astype(jnp.bfloat16)
        ratio = moment / correct_one / (jnp.sqrt(square / correct_two) + adam_eps)
        weights = master_weights[layer_index]
        results = (weights - learn_rate * (decay_rate * weights + ratio), moment_out, square_out)
        outs_weights.append(results[0])
        outs_mcode.append(results[1])
        outs_scode.append(results[2])
        outs_mscale.append(moment_max)
        outs_sscale.append(square_max)
    return (
        jnp.stack(outs_weights),
        jnp.stack(outs_mcode),
        jnp.stack(outs_scode),
        jnp.stack(outs_mscale),
        jnp.stack(outs_sscale),
    )


def solution(mesh):
    in_specs = (
        P(None, "dp", "col"),
        P(None, "dp", None),
        P(None, "dp", "col"),
        P(None, "dp", "col"),
        P(None, "dp", "col"),
        P(None, "dp", None),
        P(None, "dp", None),
    )
    out_specs = (
        P(None, "dp", "col"),
        P(None, "dp", "col"),
        P(None, "dp", "col"),
        P(None, "dp", None),
        P(None, "dp", None),
    )
    return jax.shard_map(functools.partial(local, dict(mesh.shape)), mesh=mesh, in_specs=in_specs, out_specs=out_specs, check_vma=False)
```
